256 devices in a mesh: grp: 2 (over z), bl: 128 (over x, y, core).
Axes of the slice: x: 8, y: 8, z: 2, core: 2. Of those that a mesh axis runs over, the one named last changes fastest.
The devices are a block of a 8x8x16 slice.
Arguments:
- vis: float32 [256, 512, 4, 128], P(('grp', 'bl')), parts along dimension 0, may hold values from -6 to 6
- sample_importance: float32 [256, 512], P(('grp', 'bl')), parts along dimension 0, may hold values from 0.1 to 1
- cells: int32 [256, 512, 64], P(('grp', 'bl')), parts along dimension 0, may hold values from 0 to 8191
- jones: float32 [512, 4, 128], replicated, may hold values from -3 to 3
- pairs: int32 [4, 512], P('grp'), parts along dimension 0, may hold values from 0 to 511
- pair_sequence: int32 [1024], P('grp'), parts along dimension 0, may hold values from 0 to 511, each once
Outputs:
- sky_grid: float32 [256, 4, 128], P(('grp', 'bl')), parts along dimension 0
- baseline_means: float32 [1024, 4, 128], P(('grp', 'bl')), parts along dimension 0
The draws below stay inside these ranges and needn't reach their ends.
There are 2 independent parts, one for each index of `grp`. The reference program is written for one: setup_inputs(seed, part) draws one part's arguments, and reference() takes and returns one part's arrays. A program takes and returns all parts, laid end to end along the dimension named above; an argument that names none is the same for every part. Nothing has to cross between parts.
Inputs may be any that keep to these rules, and one draw needn't show every extreme that they name: `pair_sequence`: each baseline appears once.
All inputs are finite; a program needn't handle non-finite values.
Results may differ from the reference program's by a relative error of at most 0.005.
Values sent between devices are 32-bit elements; how exact they have to be, the bound alone decides.
A program may use at most 128 MiB of HBM per device.

```python
import math
import jax
import jax.numpy as jnp
from jax import lax

ANTENNA_COUNT = 512
CHANNEL_COUNT = 64
GRID_V_CELLS = 64
TIME_TOTAL = 128
BASELINE_TOTAL = 512
GRID_U_CELLS = 128
CELL_TOTAL = 8192


def set_ends(values, key, smallest, largest):
    longest = values.shape.index(max(values.shape))
    spots = []
    for shift in (0, 1):
        where = [jax.random.randint(jax.random.fold_in(key, axis), (), 0, length) for axis, length in enumerate(values.shape)]
        where[longest] = (where[longest] + shift) % values.shape[longest]
        spots.append(tuple(where))
    return values.at[spots[0]].set(smallest).at[spots[1]].set(largest)


def levels(own_key, shape, cuts, smallest, high):
    def one(position, shards_of):
        heights = jax.random.uniform(jax.random.fold_in(jax.random.fold_in(own_key, 6), position), (shards_of,), jnp.float32, smallest / len(cuts), high / len(cuts))
        return jnp.repeat(jnp.exp(heights), shape[position] // shards_of).reshape((-1,) + (1,) * (len(shape) - position - 1))

    factor_of = one(*cuts[0])
    for cut in cuts[1:]:
        factor_of = factor_of * one(*cut)
    return factor_of


def gaussian(key, shape, scale, bound, pieces=(), kind=jnp.bfloat16):
    gain = levels(key, shape, pieces, -0.22, 0.18) if pieces else 1.0
    values = jax.random.normal(key, shape, jnp.float32) * scale * gain
    return jnp.minimum(jnp.maximum(values, -bound), bound).astype(kind)


def setup_inputs(seed: int = 0, part: int = 0) -> dict:
    splits = jax.random.split(jax.random.key(seed), 7)
    part_splits = jax.random.split(jax.random.fold_in(splits[6], part), 7)
    vis = gaussian(part_splits[0], (TIME_TOTAL, BASELINE_TOTAL, 4, 2 * CHANNEL_COUNT), 1.0, 6.0, ((0, 128),), jnp.float32)
    sample_importance = jnp.clip(jnp.exp(math.log(1.0) - 2.3025851 * jax.random.uniform(part_splits[1], (TIME_TOTAL, BASELINE_TOTAL), jnp.float32) ** levels(part_splits[1], (TIME_TOTAL, BASELINE_TOTAL), ((0, 128),), -0.2, 0.2)), 0.1, 1.0)
    cells = set_ends(jax.random.randint(part_splits[2], (TIME_TOTAL, BASELINE_TOTAL, CHANNEL_COUNT), 0, CELL_TOTAL), jax.random.fold_in(part_splits[2], 1), 0, CELL_TOTAL - 1).astype(jnp.int32)
    jones = gaussian(splits[3], (ANTENNA_COUNT, 4, 2 * CHANNEL_COUNT), 0.5, 3.0, (), jnp.float32)
    pairs = set_ends(jax.random.randint(part_splits[4], (2, BASELINE_TOTAL), 0, ANTENNA_COUNT), jax.random.fold_in(part_splits[4], 1), 0, ANTENNA_COUNT - 1).astype(jnp.int32)
    pair_sequence = jax.random.permutation(part_splits[5], BASELINE_TOTAL).astype(jnp.int32)
    return dict(vis=vis, sample_importance=sample_importance, cells=cells, jones=jones, pairs=pairs, pair_sequence=pair_sequence)


def select_part(source, index):
    half_width = source.shape[-1] // 2
    return (source[..., index, :half_width], source[..., index, half_width:])

def stokes_from(visibility, first_gain, second_gain):
    halfway = []
    for outer in range(2):
        for column in range(2):
            accum_real = 0.0
            accum_imag = 0.0
            for middle in range(2):
                gain_real, gain_imag = select_part(first_gain, 2 * outer + middle)
                data_real, data_imag = select_part(visibility, 2 * middle + column)
                accum_real = accum_real + gain_real * data_real - gain_imag * data_imag
                accum_imag = accum_imag + gain_real * data_imag + gain_imag * data_real
            halfway.append((accum_real, accum_imag))
    result = []
    for outer in range(2):
        for column in range(2):
            accum_real = 0.0
            accum_imag = 0.0
            for middle in range(2):
                left_real, left_imag = halfway[2 * outer + middle]
                gain_real, gain_imag = select_part(second_gain, 2 * column + middle)
                accum_real = accum_real + left_real * gain_real + left_imag * gain_imag
                accum_imag = accum_imag + left_imag * gain_real - left_real * gain_imag
            result.append((accum_real, accum_imag))
    stokes_real = [0.5 * (result[0][0] + result[3][0]), 0.5 * (result[0][0] - result[3][0]), 0.5 * (result[1][0] + result[2][0]), 0.5 * (result[1][1] - result[2][1])]
    stokes_imag = [0.5 * (result[0][1] + result[3][1]), 0.5 * (result[0][1] - result[3][1]), 0.5 * (result[1][1] + result[2][1]), -0.5 * (result[1][0] - result[2][0])]
    return jnp.concatenate([jnp.stack(stokes_real, -2), jnp.stack(stokes_imag, -2)], -1)

def reference(vis, sample_importance, cells, jones, pairs, pair_sequence):
    first_gain = jnp.take(jones, pairs[0], axis=0)[None]
    second_gain = jnp.take(jones, pairs[1], axis=0)[None]
    stokes = stokes_from(vis, first_gain, second_gain)
    weight_total = lax.optimization_barrier(jnp.sum(sample_importance, axis=0))
    means = lax.optimization_barrier(jnp.sum(sample_importance[:, :, None, None] * stokes, axis=0)) / weight_total[:, None, None]
    baseline_means = jnp.take(means, pair_sequence, axis=0)
    leftover_rows = (sample_importance[:, :, None, None] * (stokes - means[None])).astype(jnp.bfloat16)
    flattened_rows = leftover_rows.reshape(TIME_TOTAL, BASELINE_TOTAL, 4, 2, CHANNEL_COUNT).transpose(0, 1, 4, 2, 3).reshape(-1, 8).astype(jnp.float32)
    summed = jax.ops.segment_sum(flattened_rows, cells.reshape(-1), num_segments=GRID_U_CELLS * GRID_V_CELLS)
    grid = summed.reshape(GRID_U_CELLS, GRID_V_CELLS, 4, 2).transpose(0, 2, 3, 1).reshape(GRID_U_CELLS, 4, 2 * GRID_V_CELLS)
    scale_factor = math.sqrt(GRID_U_CELLS * GRID_V_CELLS / (TIME_TOTAL * BASELINE_TOTAL * CHANNEL_COUNT))
    return (grid * scale_factor, baseline_means)
```

```python
import functools
import math

import jax
import jax.numpy as jnp
from jax import lax
from jax.experimental import pallas as pl
from jax.experimental.pallas import tpu as pltpu
from jax.sharding import PartitionSpec as P

SUB, LANE = 8, 128
NT = (((1,), (1,)), ((), ()))

def half_pair(x0, x1, low):
    r0 = pltpu.roll(x0, 64, 1); r1 = pltpu.roll(x1, 64, 1)
    return jnp.where(low, x0, r1), jnp.where(low, r0, x1)

def interleave(x):
    row = lax.broadcasted_iota(jnp.int32, x.shape, 0)
    lane = lax.broadcasted_iota(jnp.int32, x.shape, 1)
    z = pltpu.roll(pltpu.roll(x, 4, 0), 64, 1)
    return jnp.where((row < 4) == (lane < 64), x, z)

def stage_gather(vis, jones, seq, pairs, w, cells_t, V, G, Q, CB, CR, WR, XU):
    nb = vis.shape[0] // 4
    for j in range(nb // 128):
        blk = cells_t[:, 128 * j:128 * (j + 1)]
        CB[128 * j:128 * (j + 1), :] = jnp.transpose(jnp.concatenate([blk, blk], 0))
    low = lax.broadcasted_iota(jnp.int32, (1, LANE), 1) < 64
    def body(r, _):
        half = nb // 4
        chip = lax.rem(r, half) // 2
        pair = 4 * chip + 2 * (r // half) + lax.rem(r, 2)
        b0 = seq[2 * pair]; b1 = seq[2 * pair + 1]
        for h, b in ((0, b0), (1, b1)):
            o = pl.multiple_of(8 * r + 4 * h, 4)
            V[pl.ds(o, 4), :] = vis[pl.ds(pl.multiple_of(4 * b, 4), 4), :]
            G[pl.ds(o, 4), :] = jones[pl.ds(pl.multiple_of(4 * pairs[0, b], 4), 4), :]
            Q[pl.ds(o, 4), :] = jones[pl.ds(pl.multiple_of(4 * pairs[1, b], 4), 4), :]
        cell = jnp.where(low, CB[pl.ds(b0, 1), :], CB[pl.ds(b1, 1), :])
        weight = jnp.where(low, w[b0], w[b1])
        CR[pl.ds(r, 1), :] = cell
        WR[pl.ds(r, 1), :] = weight
        row = 4 * (r // 2) + lax.rem(r, 2)
        XU[pl.ds(row, 1), :] = cell.astype(jnp.float32)
        XU[pl.ds(row + 2, 1), :] = weight
        return 0
    lax.fori_loop(0, nb // 2, body, 0, unroll=8)

def stage_stokes(V, G, Q, WR, VAL, place):
    ng = V.shape[0] // 64
    low = lax.broadcasted_iota(jnp.int32, (SUB, LANE), 1) < 64
    def body(g, _):
        def ld(ref, c):
            b = pl.multiple_of(64 * g, 64)
            return half_pair(ref[pl.ds(b + c, 8, stride=8), :], ref[pl.ds(b + 4 + c, 8, stride=8), :], low)
        v = [ld(V, c) for c in range(4)]
        gp = [ld(G, c) for c in range(4)]
        gq = [ld(Q, c) for c in range(4)]
        W = []
        for o in range(2):
            for c in range(2):
                ar = ai = 0.0
                for m in range(2):
                    gr, gi = gp[2 * o + m]; dr, di = v[2 * m + c]
                    ar = ar + gr * dr - gi * di
                    ai = ai + gr * di + gi * dr
                W.append((ar, ai))
        C = []
        for o in range(2):
            for c in range(2):
                ar = ai = 0.0
                for m in range(2):
                    lr, li = W[2 * o + m]; gr, gi = gq[2 * c + m]
                    ar = ar + lr * gr + li * gi
                    ai = ai + li * gr - lr * gi
                C.append((ar, ai))
        wh = 0.5 * WR[pl.ds(pl.multiple_of(8 * g, 8), 8), :]
        comps = [C[0][0] + C[3][0], C[0][0] - C[3][0], C[1][0] + C[2][0], C[1][1] - C[2][1],
                 C[0][1] + C[3][1], C[0][1] - C[3][1], C[1][1] + C[2][1], C[2][0] - C[1][0]]
        for j, x in enumerate(comps):
            place(VAL, g, j, wh * x)
        return 0
    lax.fori_loop(0, ng, body, 0)

def grid_rows(rows, val_of, cell_of, A, B, ACC, per):
    pos = lax.broadcasted_iota(jnp.int32, (16, LANE), 0).astype(jnp.float32).astype(jnp.bfloat16)
    def step(s, _):
        for q in range(per):
            r = s * per + q
            val = val_of(r)
            hi = val.astype(jnp.bfloat16)
            lo = (val - hi.astype(jnp.float32)).astype(jnp.bfloat16)
            both = jnp.concatenate([hi, lo], 0)
            cell = cell_of(r)
            top = cell >> 8
            bot = cell & 255
            topb = jnp.broadcast_to(top.astype(jnp.float32), (16, LANE)).astype(jnp.bfloat16)
            botb = jnp.broadcast_to(bot.astype(jnp.float32), (16, LANE)).astype(jnp.bfloat16)
            zero = jnp.zeros((16, LANE), jnp.bfloat16)
            one = jnp.ones((16, LANE), jnp.bfloat16)
            for i in range(32):
                A[16 * i:16 * i + 16, LANE * q:LANE * (q + 1)] = jnp.where(topb == jnp.bfloat16(i), both, zero)
            rel = botb - pos
            for n in range(16):
                B[16 * n:16 * n + 16, LANE * q:LANE * (q + 1)] = jnp.where(rel == jnp.bfloat16(16 * n), one, zero)
        ACC[...] += lax.dot_general(A[...], B[...], NT, preferred_element_type=jnp.float32)
        return 0
    lax.fori_loop(0, rows // per, step, 0)


MESH = pl.DeviceIdType.MESH
SMEM = pl.BlockSpec(memory_space=pltpu.SMEM)
VMEM = pl.BlockSpec(memory_space=pltpu.VMEM)
F32 = jnp.float32
BF16 = jnp.bfloat16
CELLS = 64
PER = 16
LIMIT = 60 * 1024 * 1024


def place(val, g, j, x):
    val[pl.ds(pl.multiple_of(64 * g, 64) + j, 8, stride=8), :] = x


def local_kernel(seq, pairs, w, vis, jones, cells_t, val, xu, acc, V, G, Q, CB, CR, WR, A, B):
    stage_gather(vis, jones, seq, pairs, w, cells_t, V, G, Q, CB, CR, WR, xu)
    stage_stokes(V, G, Q, WR, val, place)
    acc[...] = jnp.zeros_like(acc)
    grid_rows(
        CR.shape[0],
        lambda r: val[pl.ds(pl.multiple_of(8 * r, 8), 8), :],
        lambda r: CR[pl.ds(r, 1), :],
        A, B, acc, PER,
    )


def greet(n, me):
    barrier = pltpu.get_barrier_semaphore()

    def hello(k, _):
        pl.semaphore_signal(barrier, inc=1, device_id={"bl": lax.rem(me + k, n)}, device_id_type=MESH)
        return 0

    lax.fori_loop(1, n, hello, 0)
    pl.semaphore_wait(barrier, n - 1)


def remote(src, dst, send, recv, d):
    return pltpu.make_async_remote_copy(
        src_ref=src, dst_ref=dst, send_sem=send, recv_sem=recv, device_id={"bl": d}, device_id_type=MESH
    )


def sums_kernel(n, side, val, xu, out, xr, R1, SA, SB, RA, RB, TA, TB, UA, UB, send, recv):
    me = lax.axis_index("bl")
    core = lax.rem(me, 2)
    chip = me // 2
    x = chip // side
    y = lax.rem(chip, side)
    greet(n, me)

    first = remote(val.at[1 - core], R1, send.at[0], recv.at[0], 2 * chip + 1 - core)
    first.start()

    def deal(k, _):
        d = lax.rem(me + k, n)
        remote(xu.at[lax.rem(d, 2), d // 2], xr.at[me], send.at[1], recv.at[1], d).start()
        return 0

    lax.fori_loop(1, n, deal, 0)
    xr[me] = xu[core, chip]
    first.wait()

    def fold(i, _):
        a = i // side
        b = lax.rem(i, side)
        SA[a, b] = val[core, i, 0:8] + R1[i, 0:8]
        SB[b, a] = val[core, i, 8:16] + R1[i, 8:16]
        return 0

    lax.fori_loop(0, side * side, fold, 0, unroll=8)
    for k in range(1, side):
        xk = lax.rem(x + k, side)
        yk = lax.rem(y + k, side)
        remote(SA.at[xk], RA.at[k - 1], send.at[2], recv.at[2], (xk * side + y) * 2 + core).start()
        remote(SB.at[yk], RB.at[k - 1], send.at[3], recv.at[3], (x * side + yk) * 2 + core).start()
    remote(RA, RA, send.at[2], recv.at[2], me).wait_recv()
    remote(RB, RB, send.at[3], recv.at[3], me).wait_recv()
    for k in range(side):
        ta = SA[x, k]
        tb = SB[y, k]
        for m in range(side - 1):
            ta = ta + RA[m, k]
            tb = tb + RB[m, k]
        TA[k] = ta
        TB[k] = tb
    for k in range(1, side):
        xk = lax.rem(x + k, side)
        yk = lax.rem(y + k, side)
        remote(TA.at[yk], UA.at[k - 1], send.at[4], recv.at[4], (x * side + yk) * 2 + core).start()
        remote(TB.at[xk], UB.at[k - 1], send.at[5], recv.at[5], (xk * side + y) * 2 + core).start()
    remote(UA, UA, send.at[4], recv.at[4], me).wait_recv()
    remote(UB, UB, send.at[5], recv.at[5], me).wait_recv()
    out[0:8] = TA[y] + jnp.sum(UA[...], axis=0)
    out[8:16] = TB[x] + jnp.sum(UB[...], axis=0)
    remote(xr.at[1:n], xr.at[1:n], send.at[1], recv.at[1], me).wait_recv()
    remote(xr.at[1:n], xr.at[1:n], send.at[1], recv.at[1], me).wait_send()
    remote(RA, RA, send.at[2], recv.at[2], me).wait_send()
    remote(RB, RB, send.at[3], recv.at[3], me).wait_send()
    remote(UA, UA, send.at[4], recv.at[4], me).wait_send()
    remote(UB, UB, send.at[5], recv.at[5], me).wait_send()


def mean_kernel(n, scale, sums, xr, acc_in, grid, means, acc, MN, XC, XW, A, B):
    acc[...] = acc_in[...]
    for j in range(2):
        XC[j] = xr[:, j, :].astype(jnp.int32)
        XW[j] = xr[:, 2 + j, :]
        m = sums[8 * j:8 * j + 8, :] / jnp.sum(XW[j], axis=0, keepdims=True)
        MN[j] = -m
        y = interleave(m)
        means[2 * j] = y[0:4]
        means[2 * j + 1] = y[4:8]
    for j in range(2):
        grid_rows(
            n,
            lambda t: MN[j] * XW[j, pl.ds(t, 1), :],
            lambda t: XC[j, pl.ds(t, 1), :],
            A, B, acc, PER,
        )

    for i in range(32):
        for h in range(2):
            s = slice(128 * h, 128 * h + 128)
            y = interleave(acc[16 * i:16 * i + 8, s] + acc[16 * i + 8:16 * i + 16, s]) * scale
            grid[4 * i + 2 * h] = y[0:4]
            grid[4 * i + 2 * h + 1] = y[4:8]


def gather_kernel(n, grid, out, buf, send, recv):
    me = lax.axis_index("bl")
    greet(n, me)

    def deal(k, _):
        d = lax.rem(me + k, n)
        remote(grid.at[d], buf.at[me], send, recv, d).start()
        return 0

    lax.fori_loop(1, n, deal, 0)
    buf[me] = grid[me]
    remote(buf.at[1:n], buf.at[1:n], send, recv, me).wait_recv()
    out[0] = jnp.sum(buf[...], axis=0)
    remote(buf.at[1:n], buf.at[1:n], send, recv, me).wait_send()


def per_device(n, vis, weight, cells, jones, pairs, seq):
    side = math.isqrt(n // 2)
    nb = weight.shape[1]
    rows = nb // 2
    chans = cells.shape[2]
    sds = jax.ShapeDtypeStruct
    vm = pltpu.VMEM
    val, xu, acc = pl.pallas_call(
        local_kernel,
        out_shape=(sds((4 * nb, 128), F32), sds((4 * n, 128), F32), sds((512, 256), F32)),
        in_specs=[SMEM, SMEM, SMEM, VMEM, VMEM, VMEM],
        out_specs=(VMEM, VMEM, VMEM),
        scratch_shapes=[vm((4 * nb, 128), F32)] * 3
        + [
            vm((nb, 128), jnp.int32),
            vm((rows, 128), jnp.int32),
            vm((rows, 128), F32),
            vm((512, 128 * PER), BF16),
            vm((256, 128 * PER), BF16),
        ],
        compiler_params=pltpu.CompilerParams(vmem_limit_bytes=LIMIT),
    )(seq, pairs, weight[0], vis.reshape(4 * nb, 128), jones.reshape(-1, 128), jnp.swapaxes(cells[0], 0, 1))
    sq = side * side
    sums, xr = pl.pallas_call(
        functools.partial(sums_kernel, n, side),
        out_shape=(sds((16, 128), F32), sds((n, 4, 128), F32)),
        in_specs=[VMEM, VMEM],
        out_specs=(VMEM, VMEM),
        scratch_shapes=[
            vm((sq, 16, 128), F32),
            vm((side, side, 8, 128), F32),
            vm((side, side, 8, 128), F32),
            vm((side - 1, side, 8, 128), F32),
            vm((side - 1, side, 8, 128), F32),
            vm((side, 8, 128), F32),
            vm((side, 8, 128), F32),
            vm((side - 1, 8, 128), F32),
            vm((side - 1, 8, 128), F32),
            pltpu.SemaphoreType.DMA((6,)),
            pltpu.SemaphoreType.DMA((6,)),
        ],
        compiler_params=pltpu.CompilerParams(collective_id=0, has_side_effects=True),
    )(val.reshape(2, sq, 16, 128), xu.reshape(2, sq, 4, 128))
    scale = math.sqrt(n * CELLS / (n * nb * chans))
    grid, means = pl.pallas_call(
        functools.partial(mean_kernel, n, scale),
        out_shape=(sds((n, 4, 128), F32), sds((4, 4, 128), F32)),
        in_specs=[VMEM, VMEM, VMEM],
        out_specs=(VMEM, VMEM),
        scratch_shapes=[
            vm((512, 256), F32),
            vm((2, 8, 128), F32),
            vm((2, n, 128), jnp.int32),
            vm((2, n, 128), F32),
            vm((512, 128 * PER), BF16),
            vm((256, 128 * PER), BF16),
        ],
        compiler_params=pltpu.CompilerParams(vmem_limit_bytes=LIMIT),
    )(sums, xr, acc)
    sky = pl.pallas_call(
        functools.partial(gather_kernel, n),
        out_shape=sds((1, 4, 128), F32),
        in_specs=[VMEM],
        out_specs=VMEM,
        scratch_shapes=[vm((n, 4, 128), F32), pltpu.SemaphoreType.DMA, pltpu.SemaphoreType.DMA],
        compiler_params=pltpu.CompilerParams(collective_id=1, has_side_effects=True),
    )(grid)
    return sky, means


def solution(mesh):
    both = ("grp", "bl")
    return jax.shard_map(
        functools.partial(per_device, mesh.shape["bl"]),
        mesh=mesh,
        in_specs=(P(both, None, None, None), P(both, None), P(both, None, None), P(), P("grp", None), P("grp")),
        out_specs=(P(both, None, None), P(both, None, None)),
        check_vma=False,
    )
```

```python
import functools
import math

import jax
import jax.numpy as jnp
from jax import lax
from jax.experimental import pallas as pl
from jax.experimental.pallas import tpu as pltpu
from jax.sharding import PartitionSpec as P

MESH = pl.DeviceIdType.MESH
SMEM = pl.BlockSpec(memory_space=pltpu.SMEM)
VMEM = pl.BlockSpec(memory_space=pltpu.VMEM)
F32 = jnp.float32
BF16 = jnp.bfloat16
I32 = jnp.int32
V_CELLS = 64
LANE = 128
TOPS = 32
BOTS = 256
PER = 16
LIMIT = 60 * 1024 * 1024
NT = (((1,), (1,)), ((), ()))


def half_pair(x0, x1, low):
    r0 = pltpu.roll(x0, 64, 1)
    r1 = pltpu.roll(x1, 64, 1)
    return jnp.where(low, x0, r1), jnp.where(low, r0, x1)


def interleave(x):
    row = lax.broadcasted_iota(I32, x.shape, 0)
    lane = lax.broadcasted_iota(I32, x.shape, 1)
    z = pltpu.roll(pltpu.roll(x, 4, 0), 64, 1)
    return jnp.where((row < 4) == (lane < 64), x, z)


def slot_pair(r, nb):
    half = nb // 4
    core, chip, j = r // half, lax.rem(r, half) // 2, lax.rem(r, 2)
    return core, chip, j, 4 * chip + 2 * core + j


def stage_cells(side, seq, w, cells_t, CB, CR, WR, XU):
    nb = seq.shape[0]
    for j in range(nb // LANE):
        blk = cells_t[:, LANE * j:LANE * (j + 1)]
        CB[LANE * j:LANE * (j + 1), :] = jnp.transpose(jnp.concatenate([blk, blk], 0))
    low = lax.broadcasted_iota(I32, (1, LANE), 1) < 64

    def body(r, _):
        core, chip, j, pair = slot_pair(r, nb)
        b0 = seq[2 * pair]
        b1 = seq[2 * pair + 1]
        cell = jnp.where(low, CB[pl.ds(b0, 1), :], CB[pl.ds(b1, 1), :])
        weight = jnp.where(low, w[b0], w[b1])
        CR[pl.ds(r, 1), :] = cell
        WR[pl.ds(r, 1), :] = weight
        XU[core, j, chip // side, lax.rem(chip, side)] = jnp.concatenate([cell.astype(F32), weight], 0)
        return 0

    lax.fori_loop(0, nb // 2, body, 0, unroll=8)


def stage_rows(seq, pairs, vis, jones, V, G, Q):
    nb = seq.shape[0]

    def body(r, _):
        pair = slot_pair(r, nb)[3]
        for h in range(2):
            b = seq[2 * pair + h]
            o = pl.multiple_of(8 * r + 4 * h, 4)
            V[pl.ds(o, 4), :] = vis[pl.ds(pl.multiple_of(4 * b, 4), 4), :]
            G[pl.ds(o, 4), :] = jones[pl.ds(pl.multiple_of(4 * pairs[0, b], 4), 4), :]
            Q[pl.ds(o, 4), :] = jones[pl.ds(pl.multiple_of(4 * pairs[1, b], 4), 4), :]
        return 0

    lax.fori_loop(0, nb // 2, body, 0, unroll=8)


def stage_stokes(V, G, Q, WR, VAL):
    low = lax.broadcasted_iota(I32, (8, LANE), 1) < 64

    def body(g, _):
        base = pl.multiple_of(64 * g, 64)

        def ld(ref, c):
            return half_pair(ref[pl.ds(base + c, 8, stride=8), :], ref[pl.ds(base + 4 + c, 8, stride=8), :], low)

        v = [ld(V, c) for c in range(4)]
        gp = [ld(G, c) for c in range(4)]
        gq = [ld(Q, c) for c in range(4)]
        W = []
        for o in range(2):
            for c in range(2):
                ar = ai = 0.0
                for m in range(2):
                    gr, gi = gp[2 * o + m]
                    dr, di = v[2 * m + c]
                    ar = ar + gr * dr - gi * di
                    ai = ai + gr * di + gi * dr
                W.append((ar, ai))
        C = []
        for o in range(2):
            for c in range(2):
                ar = ai = 0.0
                for m in range(2):
                    lr, li = W[2 * o + m]
                    gr, gi = gq[2 * c + m]
                    ar = ar + lr * gr + li * gi
                    ai = ai + li * gr - lr * gi
                C.append((ar, ai))
        wh = 0.5 * WR[pl.ds(pl.multiple_of(8 * g, 8), 8), :]
        comps = [
            C[0][0] + C[3][0],
            C[0][0] - C[3][0],
            C[1][0] + C[2][0],
            C[1][1] - C[2][1],
            C[0][1] + C[3][1],
            C[0][1] - C[3][1],
            C[1][1] + C[2][1],
            C[2][0] - C[1][0],
        ]
        for j, x in enumerate(comps):
            VAL[pl.ds(base + j, 8, stride=8), :] = wh * x
        return 0

    lax.fori_loop(0, VAL.shape[0] // 64, body, 0)


def build(first, val_of, cell_of, A, B):
    pos = lax.broadcasted_iota(I32, (16, LANE), 0).astype(F32).astype(BF16)
    zero = jnp.zeros((16, LANE), BF16)
    one = jnp.ones((16, LANE), BF16)
    for q in range(PER):
        s = slice(LANE * q, LANE * (q + 1))
        val = val_of(first + q)
        hi = val.astype(BF16)
        lo = (val - hi.astype(F32)).astype(BF16)
        both = jnp.concatenate([hi, lo], 0)
        cell = cell_of(first + q)
        top = jnp.broadcast_to((cell >> 8).astype(F32), (16, LANE)).astype(BF16)
        rel = jnp.broadcast_to((cell & 255).astype(F32), (16, LANE)).astype(BF16) - pos
        for i in range(TOPS):
            A[16 * i:16 * i + 16, s] = jnp.where(top == BF16(i), both, zero)
        for i in range(BOTS // 16):
            B[16 * i:16 * i + 16, s] = jnp.where(rel == BF16(16 * i), one, zero)


def add_rows(first, rows, val_of, cell_of, A, B, ACC):
    def dot(p):
        ACC[...] += lax.dot_general(A[p][...], B[p][...], NT, preferred_element_type=F32)

    def step(s, _):
        base = first + 2 * PER * s
        build(base + PER, val_of, cell_of, A[1], B[1])
        dot(0)
        build(base + 2 * PER, val_of, cell_of, A[0], B[0])
        dot(1)
        return 0

    lax.fori_loop(0, rows // (2 * PER), step, 0)


def remote(src, dst, send, recv, i, d):
    return pltpu.make_async_remote_copy(
        src_ref=src,
        dst_ref=dst,
        send_sem=send.at[i],
        recv_sem=recv.at[i],
        device_id={"bl": d},
        device_id_type=MESH,
    )


def local_kernel(side, seq, pairs, w, vis, jones, cells_t, VAL, CR, XU, V, G, Q, CB, WR):
    stage_cells(side, seq, w, cells_t, CB, CR, WR, XU)
    stage_rows(seq, pairs, vis, jones, V, G, Q)
    stage_stokes(V, G, Q, WR, VAL)


def whole_kernel(n, side, scale, VAL, CR, XU, sky, means,
                 PX, XA, XB, YA, YB, R1, SA, SB, RA, RB, TA, TB, UA, UB,
                 ACC, MN, A0, B0, A1, B1, GR, PG, GA, GB, HA, HB, KA, KB, LA, LB, send, recv):
    me = lax.axis_index("bl")
    core = lax.rem(me, 2)
    chip = me // 2
    x = chip // side
    y = lax.rem(chip, side)
    mate = 2 * chip + 1 - core
    half = 8 * side * side * 2
    ring = [(lax.rem(x + k, side), lax.rem(y + k, side)) for k in range(1, side)]

    def at_x(xk):
        return (xk * side + y) * 2 + core

    def at_y(yk):
        return (x * side + yk) * 2 + core

    def landed(ref, i):
        remote(ref, ref, send, recv, i, mate).wait_recv()

    def sent(ref, i):
        remote(ref, ref, send, recv, i, mate).wait_send()

    barrier = pltpu.get_barrier_semaphore()
    for xk, yk in ring:
        pl.semaphore_signal(barrier, inc=1, device_id={"bl": at_x(xk)}, device_id_type=MESH)
        pl.semaphore_signal(barrier, inc=1, device_id={"bl": at_y(yk)}, device_id_type=MESH)
    pl.semaphore_signal(barrier, inc=1, device_id={"bl": mate}, device_id_type=MESH)

    pl.semaphore_wait(barrier, 2 * side - 1)
    remote(VAL.at[pl.ds(pl.multiple_of((1 - core) * half, half), half)], R1, send, recv, 5, mate).start()
    remote(XU.at[1 - core], PX, send, recv, 0, mate).start()

    rows = CR.shape[0]

    def own_val(r):
        return VAL[pl.ds(pl.multiple_of(8 * lax.rem(r, rows), 8), 8), :]

    def own_cell(r):
        return CR[pl.ds(lax.rem(r, rows), 1), :]

    bufs = (A0, A1), (B0, B1)
    ACC[...] = jnp.zeros_like(ACC)
    build(0, own_val, own_cell, A0, B0)
    landed(R1, 5)

    def fold(i, _):
        a = i // side
        b = lax.rem(i, side)
        mine = pl.multiple_of(core * half + 16 * i, 16)
        other = pl.multiple_of(16 * i, 16)
        SA[a, b] = VAL[pl.ds(mine, 8), :] + R1[pl.ds(other, 8), :]
        SB[b, a] = VAL[pl.ds(mine + 8, 8), :] + R1[pl.ds(other + 8, 8), :]
        return 0

    lax.fori_loop(0, side * side, fold, 0, unroll=8)
    for k, (xk, yk) in enumerate(ring):
        remote(SA.at[xk], RA.at[k], send, recv, 6, at_x(xk)).start()
        remote(SB.at[yk], RB.at[k], send, recv, 7, at_y(yk)).start()
    landed(PX, 0)
    for k, (xk, yk) in enumerate(ring, 1):
        remote(XU.at[core, 0, xk], XA.at[0, k], send, recv, 1, at_x(xk)).start()
        remote(PX.at[0, xk], XA.at[1, k], send, recv, 1, at_x(xk)).start()
        remote(XU.at[core, 1, :, yk], XB.at[0, k], send, recv, 2, at_y(yk)).start()
        remote(PX.at[1, :, yk], XB.at[1, k], send, recv, 2, at_y(yk)).start()
    XA[0, 0] = XU[core, 0, x]
    XA[1, 0] = PX[0, x]
    XB[0, 0] = XU[core, 1, :, y]
    XB[1, 0] = PX[1, :, y]
    add_rows(0, 5 * rows // 8, own_val, own_cell, *bufs, ACC)
    landed(RA, 6)
    landed(RB, 7)
    for k in range(side):
        ta = SA[x, k]
        tb = SB[y, k]
        for m in range(side - 1):
            ta = ta + RA[m, k]
            tb = tb + RB[m, k]
        TA[k] = ta
        TB[k] = tb
    for k, (xk, yk) in enumerate(ring):
        remote(TA.at[yk], UA.at[k], send, recv, 8, at_y(yk)).start()
        remote(TB.at[xk], UB.at[k], send, recv, 9, at_x(xk)).start()
    landed(XA.at[:, 1:side], 1)
    landed(XB.at[:, 1:side], 2)
    for k, (xk, yk) in enumerate(ring, 1):
        remote(XA.at[:, :, yk], YA.at[k], send, recv, 3, at_y(yk)).start()
        remote(XB.at[:, :, xk], YB.at[k], send, recv, 4, at_x(xk)).start()
    YA[0] = XA[:, :, y]
    YB[0] = XB[:, :, x]
    add_rows(5 * rows // 8, 3 * rows // 8, own_val, own_cell, *bufs, ACC)
    landed(YA.at[1:side], 3)
    landed(YB.at[1:side], 4)
    landed(UA, 8)
    landed(UB, 9)

    for j, (t, u, at, Y) in enumerate(((TA, UA, y, YA), (TB, UB, x, YB))):
        total = t[at] + jnp.sum(u[...], axis=0)
        m = total / jnp.sum(Y[:, :, :, 1, :].reshape(n, LANE), axis=0, keepdims=True)
        MN[j] = -m
        z = interleave(m)
        means[2 * j] = z[0:4]
        means[2 * j + 1] = z[4:8]
    for j, Y in enumerate((YA, YB)):
        def sample(t, row, Y=Y):
            t = lax.rem(t, n)
            return Y[t // (2 * side), lax.rem(t, 2 * side) // side, lax.rem(t, side), pl.ds(row, 1), :]

        def mean_val(t, j=j, sample=sample):
            return MN[j] * sample(t, 1)

        def mean_cell(t, sample=sample):
            return sample(t, 0).astype(I32)

        build(0, mean_val, mean_cell, A0, B0)
        add_rows(0, n, mean_val, mean_cell, *bufs, ACC)

    for i in range(TOPS):
        for h in range(BOTS // LANE):
            s = slice(LANE * h, LANE * (h + 1))
            z = interleave(ACC[16 * i:16 * i + 8, s] + ACC[16 * i + 8:16 * i + 16, s]) * scale
            for e in range(2):
                d = 4 * i + 2 * h + e
                GR[d % 2, d // 2 // side, d // 2 % side] = z[4 * e:4 * e + 4]

    remote(GR.at[1 - core], PG, send, recv, 10, mate).start()
    landed(PG, 10)
    for a in range(side):
        z = GR[core, a] + PG[a]
        GA[a] = z[:, 0:2]
        for b in range(side):
            GB[b, a] = z[b, 2:4]
    for k, (xk, yk) in enumerate(ring):
        remote(GA.at[xk], HA.at[k], send, recv, 11, at_x(xk)).start()
        remote(GB.at[yk], HB.at[k], send, recv, 12, at_y(yk)).start()
    landed(HA, 11)
    landed(HB, 12)
    KA[...] = GA[x] + jnp.sum(HA[...], axis=0)
    KB[...] = GB[y] + jnp.sum(HB[...], axis=0)
    for k, (xk, yk) in enumerate(ring):
        remote(KA.at[yk], LA.at[k], send, recv, 13, at_y(yk)).start()
        remote(KB.at[xk], LB.at[k], send, recv, 14, at_x(xk)).start()
    landed(LA, 13)
    landed(LB, 14)
    sky[0, 0:2] = KA[y] + jnp.sum(LA[...], axis=0)
    sky[0, 2:4] = KB[x] + jnp.sum(LB[...], axis=0)
    for ref, i in (
        (PX, 0), (XA.at[:, 1:side], 1), (XB.at[:, 1:side], 2), (YA.at[1:side], 3), (YB.at[1:side], 4), (R1, 5),
        (RA, 6), (RB, 7), (UA, 8), (UB, 9), (PG, 10), (HA, 11), (HB, 12), (LA, 13), (LB, 14),
    ):
        sent(ref, i)


def per_device(n, vis, weight, cells, jones, pairs, seq):
    side = math.isqrt(n // 2)
    nb = weight.shape[1]
    rows = nb // 2
    sds = jax.ShapeDtypeStruct
    scale = math.sqrt(n * V_CELLS / (n * nb * cells.shape[2]))

    def vm(*shape, dtype=F32):
        return pltpu.VMEM(shape, dtype)

    tall = TOPS * 16
    staged = pl.pallas_call(
        functools.partial(local_kernel, side),
        out_shape=(sds((4 * nb, LANE), F32), sds((rows, LANE), I32), sds((2, 2, side, side, 2, LANE), F32)),
        in_specs=[SMEM, SMEM, SMEM, VMEM, VMEM, VMEM],
        out_specs=(VMEM, VMEM, VMEM),
        scratch_shapes=[vm(4 * nb, LANE)] * 3 + [vm(nb, LANE, dtype=I32), vm(rows, LANE)],
        compiler_params=pltpu.CompilerParams(vmem_limit_bytes=LIMIT),
    )(seq, pairs, weight[0], vis.reshape(4 * nb, LANE), jones.reshape(-1, LANE), jnp.swapaxes(cells[0], 0, 1))
    sky, means = pl.pallas_call(
        functools.partial(whole_kernel, n, side, scale),
        out_shape=(sds((1, 4, LANE), F32), sds((4, 4, LANE), F32)),
        in_specs=[VMEM, VMEM, VMEM],
        out_specs=(VMEM, VMEM),
        scratch_shapes=[vm(2, side, side, 2, LANE)]
        + [vm(2, side, side, 2, LANE)] * 2
        + [vm(side, 2, side, 2, LANE)] * 2
        + [vm(2 * nb, LANE)]
        + [vm(side, side, 8, LANE)] * 2
        + [vm(side - 1, side, 8, LANE)] * 2
        + [vm(side, 8, LANE)] * 2
        + [vm(side - 1, 8, LANE)] * 2
        + [vm(tall, BOTS), vm(2, 8, LANE)]
        + [vm(tall, LANE * PER, dtype=BF16), vm(BOTS, LANE * PER, dtype=BF16)] * 2
        + [vm(2, side, side, 4, LANE), vm(side, side, 4, LANE)]
        + [vm(side, side, 2, LANE)] * 2
        + [vm(side - 1, side, 2, LANE)] * 2
        + [vm(side, 2, LANE)] * 2
        + [vm(side - 1, 2, LANE)] * 2
        + [pltpu.SemaphoreType.DMA((15,))] * 2,
        compiler_params=pltpu.CompilerParams(collective_id=0, has_side_effects=True, vmem_limit_bytes=LIMIT),
    )(*staged)
    return sky, means


def solution(mesh):
    both = ("grp", "bl")
    return jax.shard_map(
        functools.partial(per_device, mesh.shape["bl"]),
        mesh=mesh,
        in_specs=(P(both, None, None, None), P(both, None), P(both, None, None), P(), P("grp", None), P("grp")),
        out_specs=(P(both, None, None), P(both, None, None)),
        check_vma=False,
    )
```

```python
import functools
import math

import jax
import jax.numpy as jnp
from jax import lax
from jax.experimental import pallas as pl
from jax.experimental.pallas import tpu as pltpu
from jax.sharding import PartitionSpec as P

MESH = pl.DeviceIdType.MESH
SMEM = pl.BlockSpec(memory_space=pltpu.SMEM)
HBM = pl.BlockSpec(memory_space=pltpu.HBM)
VMEM = pl.BlockSpec(memory_space=pltpu.VMEM)
F32 = jnp.float32
BF16 = jnp.bfloat16
I32 = jnp.int32
V_CELLS = 64
LANE = 128
TOPS = 32
BOTS = 256
PER = 16
EARLY = 5
MIB = 1024 * 1024
NT = (((1,), (1,)), ((), ()))


def half_pair(x0, x1, low):
    r0 = pltpu.roll(x0, 64, 1)
    r1 = pltpu.roll(x1, 64, 1)
    return jnp.where(low, x0, r1), jnp.where(low, r0, x1)


def interleave(x):
    row = lax.broadcasted_iota(I32, x.shape, 0)
    lane = lax.broadcasted_iota(I32, x.shape, 1)
    z = pltpu.roll(pltpu.roll(x, 4, 0), 64, 1)
    return jnp.where((row < 4) == (lane < 64), x, z)


def stage(side, seq, pairs, w, vis, jones, V, G, Q, CB, CR, CU, WR, WC):
    nb = seq.shape[0]
    low = lax.broadcasted_iota(I32, (1, LANE), 1) < 64

    def body(a, _):
        for core in range(2):
            for b in range(side):
                chip = side * a + b if core == 0 else a + side * b
                for j in range(2):
                    r = 2 * side * a + (nb // 4 * core + 2 * b + j)
                    slot = 8 * chip + (4 * core + 2 * j)
                    both = seq[slot], seq[slot + 1]
                    for h in range(2):
                        o = 8 * r + 4 * h
                        V[pl.ds(o, 4), :] = vis[pl.ds(4 * both[h], 4), :]
                        G[pl.ds(o, 4), :] = jones[pl.ds(4 * pairs[0, both[h]], 4), :]
                        Q[pl.ds(o, 4), :] = jones[pl.ds(4 * pairs[1, both[h]], 4), :]
                    cell = jnp.where(low, CB[pl.ds(both[0], 1), :], CB[pl.ds(both[1], 1), :])
                    CR[pl.ds(r, 1), :] = cell
                    CU[core, a, b, j:j + 1] = cell
                    WR[pl.ds(r, 1), :] = jnp.where(low, w[0, both[0]], w[0, both[1]])
        return 0

    lax.fori_loop(0, side, body, 0)
    for core in range(2):
        turned = jnp.transpose(WR[LANE * core:LANE * (core + 1), :])
        WC[core, 0:1] = turned[0:1]
        WC[core, 1:2] = turned[64:65]


def stage_stokes(V, G, Q, WR, VAL):
    low = lax.broadcasted_iota(I32, (8, LANE), 1) < 64

    def body(g, _):
        base = pl.multiple_of(64 * g, 64)

        def ld(ref, c):
            return half_pair(ref[pl.ds(base + c, 8, stride=8), :], ref[pl.ds(base + 4 + c, 8, stride=8), :], low)

        v = [ld(V, c) for c in range(4)]
        gp = [ld(G, c) for c in range(4)]
        gq = [ld(Q, c) for c in range(4)]
        W = []
        for o in range(2):
            for c in range(2):
                ar = ai = 0.0
                for m in range(2):
                    gr, gi = gp[2 * o + m]
                    dr, di = v[2 * m + c]
                    ar = ar + gr * dr - gi * di
                    ai = ai + gr * di + gi * dr
                W.append((ar, ai))
        C = []
        for o in range(2):
            for c in range(2):
                ar = ai = 0.0
                for m in range(2):
                    lr, li = W[2 * o + m]
                    gr, gi = gq[2 * c + m]
                    ar = ar + lr * gr + li * gi
                    ai = ai + li * gr - lr * gi
                C.append((ar, ai))
        wh = 0.5 * WR[pl.ds(pl.multiple_of(8 * g, 8), 8), :]
        comps = [
            C[0][0] + C[3][0],
            C[0][0] - C[3][0],
            C[1][0] + C[2][0],
            C[1][1] - C[2][1],
            C[0][1] + C[3][1],
            C[0][1] - C[3][1],
            C[1][1] + C[2][1],
            C[2][0] - C[1][0],
        ]
        for j, x in enumerate(comps):
            VAL[pl.ds(base + j, 8, stride=8), :] = wh * x
        return 0

    lax.fori_loop(0, VAL.shape[0] // 64, body, 0, unroll=4)


def build(first, val_of, cell_of, A, B):
    pos = lax.broadcasted_iota(I32, (16, LANE), 0).astype(F32).astype(BF16)
    zero = jnp.zeros((16, LANE), BF16)
    one = jnp.ones((16, LANE), BF16)
    for q in range(PER):
        s = slice(LANE * q, LANE * (q + 1))
        val = val_of(first + q)
        hi = val.astype(BF16)
        lo = (val - hi.astype(F32)).astype(BF16)
        both = jnp.concatenate([hi, lo], 0)
        cell = cell_of(first + q)
        top = jnp.broadcast_to((cell >> 8).astype(F32), (16, LANE)).astype(BF16)
        rel = jnp.broadcast_to((cell & 255).astype(F32), (16, LANE)).astype(BF16) - pos
        for i in range(TOPS):
            A[16 * i:16 * i + 16, s] = jnp.where(top == BF16(i), both, zero)
        for i in range(BOTS // 16):
            B[16 * i:16 * i + 16, s] = jnp.where(rel == BF16(16 * i), one, zero)


def add_rows(first, rows, val_of, cell_of, A, B, ACC):
    def dot(p):
        ACC[...] += lax.dot_general(A[p][...], B[p][...], NT, preferred_element_type=F32)

    def step(s, _):
        base = first + 2 * PER * s
        build(base + PER, val_of, cell_of, A[1], B[1])
        dot(0)
        build(base + 2 * PER, val_of, cell_of, A[0], B[0])
        dot(1)
        return 0

    lax.fori_loop(0, rows // (2 * PER), step, 0)


def remote(src, dst, send, recv, i, d):
    return pltpu.make_async_remote_copy(
        src_ref=src,
        dst_ref=dst,
        send_sem=send.at[i],
        recv_sem=recv.at[i],
        device_id={"bl": d},
        device_id_type=MESH,
    )


def local_kernel(side, *refs):
    outside, (VAL, CR, CU, WC), inside, (V, G, Q, CB, WR, sem) = refs[:6], refs[6:10], refs[10:16], refs[16:]
    copies = [pltpu.make_async_copy(a, b, sem.at[i]) for i, (a, b) in enumerate(zip(outside, inside))]
    for copy in copies:
        copy.start()
    seq, pairs, w, vis, jones, cells_t = inside
    copies[5].wait()
    for j in range(cells_t.shape[1] // LANE):
        blk = cells_t[:, LANE * j:LANE * (j + 1)]
        CB[LANE * j:LANE * (j + 1), :] = jnp.transpose(jnp.concatenate([blk, blk], 0))
    for copy in copies[:5]:
        copy.wait()
    stage(side, seq, pairs, w, vis, jones, V, G, Q, CB, CR, CU, WR, WC)
    stage_stokes(V, G, Q, WR, VAL)


def spread(row):
    return jnp.broadcast_to(row.astype(F32), (16, LANE)).astype(BF16)


def weigh_cells(CT, W4, HS, HB):
    pos = lax.broadcasted_iota(I32, (16, LANE), 0).astype(F32).astype(BF16)
    zero = jnp.zeros((16, LANE), BF16)
    one = jnp.ones((16, LANE), BF16)
    high = HB.shape[0]
    pitch = high + 8

    def body(g, _):
        wrow = W4[pl.ds(g // 4, 1), :]
        whi = wrow.astype(BF16)
        wlo = spread(wrow - whi.astype(F32))
        whi = spread(whi)
        for q in range(16):
            cell = CT[pl.ds(16 * g + q, 1), :]
            up = spread(cell >> 7) - pos
            along = spread(cell & 127) - pos
            hits = [up == BF16(16 * i) for i in range(high // 16)]
            left = jnp.concatenate([jnp.where(m, whi, zero) for m in hits] + [jnp.where(m, wlo, zero) for m in hits], 0)
            right = jnp.concatenate([jnp.where(along == BF16(16 * i), one, zero) for i in range(8)], 0)
            both = lax.dot_general(left, right, NT, preferred_element_type=F32)
            HS[pitch * q:pitch * q + high, :] = both[:high] + both[high:]
        for u in range(high):
            x = jnp.concatenate([HS[pl.ds(u, 8, stride=pitch), :], HS[pl.ds(u + 8 * pitch, 8, stride=pitch), :]], 0)
            hi = x.astype(BF16)
            HB[u, pl.ds(16 * g, 16), 0:LANE] = hi
            HB[u, pl.ds(16 * g, 16), LANE:2 * LANE] = (x - hi.astype(F32)).astype(BF16)
        return 0

    lax.fori_loop(0, CT.shape[0] // 16, body, 0)


def whole_kernel(n, side, scale, VAL, CR, CU, WC, sky, means, PC, PW, X, XW, Y, YW, R1, RA, T, U,
                 ACC, A0, B0, A1, B1, CT, WT, W4, HS, HB, GR, PG, HA, K, L, send, recv):
    me = lax.axis_index("bl")
    core = lax.rem(me, 2)
    chip = me // 2
    x = chip // side
    y = lax.rem(chip, side)
    mate = 2 * chip + 1 - core
    first = x + core * (y - x)
    second = y + core * (x - y)
    step1 = 2 * side + core * (2 - 2 * side)
    step2 = 2 + core * (2 * side - 2)
    rows = CR.shape[0]

    def on_first(k):
        place = lax.rem(first + k, side)
        return place, me + (place - first) * step1

    def on_second(k):
        place = lax.rem(second + k, side)
        return place, me + (place - second) * step2

    def landed(ref, i):
        remote(ref, ref, send, recv, i, mate).wait_recv()

    def sent(ref, i):
        remote(ref, ref, send, recv, i, mate).wait_send()

    barrier = pltpu.get_barrier_semaphore()
    for k in range(1, side):
        for d in (on_first(k)[1], on_second(k)[1]):
            pl.semaphore_signal(barrier, inc=1, device_id={"bl": d}, device_id_type=MESH)
    pl.semaphore_signal(barrier, inc=1, device_id={"bl": mate}, device_id_type=MESH)
    pl.semaphore_wait(barrier, 2 * side - 1)

    remote(CU.at[1 - core], PC, send, recv, 0, mate).start()
    remote(WC.at[1 - core], PW, send, recv, 3, mate).start()
    remote(VAL.at[1 - core], R1, send, recv, 6, mate).start()

    def own_val(r):
        r = lax.rem(r, rows)
        unit = r // 2
        half = rows // 4
        at = pl.multiple_of(8 * lax.rem(r, 2), 8)
        return VAL[unit // half, lax.rem(unit, half) // side, lax.rem(unit, side), pl.ds(at, 8), :]

    def own_cell(r):
        return CR[pl.ds(lax.rem(r, rows), 1), :]

    bufs = (A0, A1), (B0, B1)
    ACC[...] = jnp.zeros_like(ACC)
    build(0, own_val, own_cell, A0, B0)
    landed(PC, 0)
    landed(PW, 3)
    landed(R1, 6)

    def fold(i, _):
        R1[i] = R1[i] + VAL[core, i]
        return 0

    lax.fori_loop(0, side, fold, 0)
    for k in range(1, side):
        place, d = on_first(k)
        remote(R1.at[place], RA.at[k - 1], send, recv, 7, d).start()
    for k in range(1, side):
        place, d = on_first(k)
        remote(CU.at[core, place], X.at[0, k], send, recv, 1, d).start()
        remote(PC.at[place], X.at[1, k], send, recv, 1, d).start()
        remote(WC.at[core], XW.at[0, k], send, recv, 4, d).start()
        remote(PW, XW.at[1, k], send, recv, 4, d).start()
    X[0, 0] = CU[core, first]
    X[1, 0] = PC[first]
    XW[0, 0] = WC[core]
    XW[1, 0] = PW[...]
    add_rows(0, EARLY * rows // 8, own_val, own_cell, *bufs, ACC)
    landed(RA, 7)
    for i in range(side):
        t = R1[first, i]
        for k in range(side - 1):
            t = t + RA[k, i]
        T[i] = t
    for k in range(1, side):
        place, d = on_second(k)
        remote(T.at[place], U.at[k - 1], send, recv, 8, d).start()
    landed(X.at[:, 1:side], 1)
    landed(XW.at[:, 1:side], 4)
    for k in range(1, side):
        place, d = on_second(k)
        remote(X.at[:, :, place], Y.at[k], send, recv, 2, d).start()
        remote(XW, YW.at[k], send, recv, 5, d).start()
    Y[0] = X[:, :, second]
    YW[0] = XW[...]
    add_rows(EARLY * rows // 8, (8 - EARLY) * rows // 8, own_val, own_cell, *bufs, ACC)
    landed(Y.at[1:side], 2)
    landed(YW.at[1:side], 5)
    for j in range(2):
        CT[LANE * j:LANE * (j + 1), :] = jnp.transpose(Y[:, :, :, j, :].reshape(n, LANE))
    for h in range(2):
        WT[...] = jnp.transpose(YW[:, :, :, h, :].reshape(n, LANE))
        for j in range(2):
            W4[2 * j + h:2 * j + h + 1, :] = WT[pl.ds(2 * side * first + 2 * second + j, 1), :]
    weigh_cells(CT, W4, HS, HB)
    landed(U, 8)

    total = T[second] + jnp.sum(U[...], axis=0)
    low = lax.broadcasted_iota(I32, (1, LANE), 1) < 64
    weights = jnp.sum(W4[...], axis=1, keepdims=True)
    averages = []
    for j in range(2):
        m = total[8 * j:8 * j + 8] / jnp.where(low, weights[2 * j:2 * j + 1], weights[2 * j + 1:2 * j + 2])
        averages.append(m)
        z = interleave(m)
        means[2 * j] = z[0:4]
        means[2 * j + 1] = z[4:8]
    m = jnp.concatenate(averages, 1)
    hi = m.astype(BF16)
    lo = (m - hi.astype(F32)).astype(BF16)
    left = jnp.concatenate([hi, lo], 0)
    for u in range(HB.shape[0]):
        both = jnp.dot(left, HB[u], preferred_element_type=F32)
        both = both[0:8] + both[8:16]
        i, h = u // 2, u % 2
        s = slice(LANE * h, LANE * (h + 1))
        z = ACC[16 * i:16 * i + 8, s] + ACC[16 * i + 8:16 * i + 16, s] - (both[:, :LANE] + both[:, LANE:])
        z = interleave(z) * scale
        for e in range(2):
            d = 2 * u + e
            at = (d // 2 // side, d // 2 % side) if e == 0 else (d // 2 % side, d // 2 // side)
            GR[e, at[0], at[1]] = z[4 * e:4 * e + 4]

    remote(GR.at[1 - core], PG, send, recv, 9, mate).start()
    landed(PG, 9)
    PG[...] = PG[...] + GR[core]
    for k in range(1, side):
        place, d = on_first(k)
        remote(PG.at[place], HA.at[k - 1], send, recv, 10, d).start()
    landed(HA, 10)
    K[...] = PG[first] + jnp.sum(HA[...], axis=0)
    for k in range(1, side):
        place, d = on_second(k)
        remote(K.at[place], L.at[k - 1], send, recv, 11, d).start()
    landed(L, 11)
    sky[0] = K[second] + jnp.sum(L[...], axis=0)
    for ref, i in (
        (PC, 0), (X.at[:, 1:side], 1), (Y.at[1:side], 2), (PW, 3), (XW.at[:, 1:side], 4), (YW.at[1:side], 5),
        (R1, 6), (RA, 7), (U, 8), (PG, 9), (HA, 10), (L, 11),
    ):
        sent(ref, i)


def per_device(n, vis, weight, cells, jones, pairs, seq):
    side = math.isqrt(n // 2)
    nb = weight.shape[1]
    rows = nb // 2
    sds = jax.ShapeDtypeStruct
    scale = math.sqrt(n * V_CELLS / (n * nb * cells.shape[2]))

    def vm(*shape, dtype=F32):
        return pltpu.VMEM(shape, dtype)

    tall = TOPS * 16
    val, *staged = pl.pallas_call(
        functools.partial(local_kernel, side),
        out_shape=(
            sds((4 * nb, LANE), F32),
            sds((rows, LANE), I32),
            sds((2, side, side, 2, LANE), I32),
            sds((2, 2, LANE), F32),
        ),
        in_specs=[HBM] * 6,
        out_specs=(VMEM,) * 4,
        scratch_shapes=[pltpu.SMEM((nb,), I32), pltpu.SMEM((2, nb), I32), pltpu.SMEM((1, nb), F32)]
        + [vm(4 * nb, LANE), vm(4 * jones.shape[0], LANE), vm(cells.shape[2], nb, dtype=I32)]
        + [vm(4 * nb, LANE)] * 3
        + [vm(nb, LANE, dtype=I32), vm(rows, LANE), pltpu.SemaphoreType.DMA((6,))],
        compiler_params=pltpu.CompilerParams(vmem_limit_bytes=12 * MIB),
    )(seq, pairs, weight, vis.reshape(4 * nb, LANE), jones.reshape(-1, LANE), jnp.swapaxes(cells[0], 0, 1))
    sky, means = pl.pallas_call(
        functools.partial(whole_kernel, n, side, scale),
        out_shape=(sds((1, 4, LANE), F32), sds((4, 4, LANE), F32)),
        in_specs=[VMEM] * 4,
        out_specs=(VMEM, VMEM),
        scratch_shapes=[vm(side, side, 2, LANE, dtype=I32), vm(2, LANE)]
        + [vm(2, side, side, 2, LANE, dtype=I32), vm(2, side, 2, LANE)]
        + [vm(side, 2, side, 2, LANE, dtype=I32), vm(side, 2, side, 2, LANE)]
        + [vm(side, side, 16, LANE), vm(side - 1, side, 16, LANE), vm(side, 16, LANE), vm(side - 1, 16, LANE)]
        + [vm(tall, BOTS)]
        + [vm(tall, LANE * PER, dtype=BF16), vm(BOTS, LANE * PER, dtype=BF16)] * 2
        + [vm(rows, LANE, dtype=I32), vm(n, LANE), vm(4, LANE)]
        + [vm(16 * (n // 2 + 8), LANE), vm(n // 2, rows, 2 * LANE, dtype=BF16)]
        + [vm(2, side, side, 4, LANE), vm(side, side, 4, LANE), vm(side - 1, side, 4, LANE)]
        + [vm(side, 4, LANE), vm(side - 1, 4, LANE)]
        + [pltpu.SemaphoreType.DMA((12,))] * 2,
        compiler_params=pltpu.CompilerParams(collective_id=0, has_side_effects=True, vmem_limit_bytes=32 * MIB),
    )(val.reshape(2, side, side, 16, LANE), *staged)
    return sky, means


def solution(mesh):
    both = ("grp", "bl")
    return jax.shard_map(
        functools.partial(per_device, mesh.shape["bl"]),
        mesh=mesh,
        in_specs=(P(both, None, None, None), P(both, None), P(both, None, None), P(), P("grp", None), P("grp")),
        out_specs=(P(both, None, None), P(both, None, None)),
        check_vma=False,
    )
```

```python
import functools
import math

import jax
import jax.numpy as jnp
from jax import lax
from jax.experimental import pallas as pl
from jax.experimental.pallas import tpu as pltpu
from jax.sharding import PartitionSpec as P

MESH = pl.DeviceIdType.MESH
SMEM = pl.BlockSpec(memory_space=pltpu.SMEM)
VMEM = pl.BlockSpec(memory_space=pltpu.VMEM)
F32 = jnp.float32
BF16 = jnp.bfloat16
I32 = jnp.int32
V_CELLS = 64
LANE = 128
TOPS = 32
BOTS = 256
PER = 16
MIB = 1024 * 1024
NT = (((1,), (1,)), ((), ()))


def half_pair(x0, x1, low):
    r0 = pltpu.roll(x0, 64, 1)
    r1 = pltpu.roll(x1, 64, 1)
    return jnp.where(low, x0, r1), jnp.where(low, r0, x1)


def interleave(x):
    row = lax.broadcasted_iota(I32, x.shape, 0)
    lane = lax.broadcasted_iota(I32, x.shape, 1)
    z = pltpu.roll(pltpu.roll(x, 4, 0), 64, 1)
    return jnp.where((row < 4) == (lane < 64), x, z)


def stage(side, seq, pairs, w, vis, jones, V, G, Q, CB, CR, CU, WR, WC):
    nb = seq.shape[0]
    low = lax.broadcasted_iota(I32, (1, LANE), 1) < 64

    def body(a, _):
        for core in range(2):
            for b in range(side):
                chip = side * a + b if core == 0 else a + side * b
                for j in range(2):
                    r = 2 * side * a + (nb // 4 * core + 2 * b + j)
                    slot = 8 * chip + (4 * core + 2 * j)
                    both = seq[slot], seq[slot + 1]
                    for h in range(2):
                        o = 8 * r + 4 * h
                        V[pl.ds(o, 4), :] = vis[pl.ds(4 * both[h], 4), :]
                        G[pl.ds(o, 4), :] = jones[pl.ds(4 * pairs[0, both[h]], 4), :]
                        Q[pl.ds(o, 4), :] = jones[pl.ds(4 * pairs[1, both[h]], 4), :]
                    cell = jnp.where(low, CB[pl.ds(both[0], 1), :], CB[pl.ds(both[1], 1), :])
                    CR[pl.ds(r, 1), :] = cell
                    CU[core, a, b, j:j + 1] = cell
                    WR[pl.ds(r, 1), :] = jnp.where(low, w[0, both[0]], w[0, both[1]])
        return 0

    lax.fori_loop(0, side, body, 0)
    for core in range(2):
        turned = jnp.transpose(WR[LANE * core:LANE * (core + 1), :])
        WC[core, 0:1] = turned[0:1]
        WC[core, 1:2] = turned[64:65]


def stage_stokes(V, G, Q, WR, WQ, VAL):
    low = lax.broadcasted_iota(I32, (8, LANE), 1) < 64

    def body(g, _):
        base = pl.multiple_of(64 * g, 64)

        def ld(ref, c):
            return half_pair(ref[pl.ds(base + c, 8, stride=8), :], ref[pl.ds(base + 4 + c, 8, stride=8), :], low)

        v = [ld(V, c) for c in range(4)]
        gp = [ld(G, c) for c in range(4)]
        gq = [ld(Q, c) for c in range(4)]
        W = []
        for o in range(2):
            for c in range(2):
                ar = ai = 0.0
                for m in range(2):
                    gr, gi = gp[2 * o + m]
                    dr, di = v[2 * m + c]
                    ar = ar + gr * dr - gi * di
                    ai = ai + gr * di + gi * dr
                W.append((ar, ai))
        C = []
        for o in range(2):
            for c in range(2):
                ar = ai = 0.0
                for m in range(2):
                    lr, li = W[2 * o + m]
                    gr, gi = gq[2 * c + m]
                    ar = ar + lr * gr + li * gi
                    ai = ai + li * gr - lr * gi
                C.append((ar, ai))
        eight = pl.ds(pl.multiple_of(8 * g, 8), 8)
        weight = WR[eight, :]
        WQ[eight, :] = weight.astype(BF16).astype(F32) / weight
        wh = 0.5 * weight
        comps = [
            C[0][0] + C[3][0],
            C[0][0] - C[3][0],
            C[1][0] + C[2][0],
            C[1][1] - C[2][1],
            C[0][1] + C[3][1],
            C[0][1] - C[3][1],
            C[1][1] + C[2][1],
            C[2][0] - C[1][0],
        ]
        for j, x in enumerate(comps):
            VAL[pl.ds(base + j, 8, stride=8), :] = wh * x
        return 0

    lax.fori_loop(0, VAL.shape[0] // 64, body, 0, unroll=4)


def build(first, val_of, cell_of, A, B):
    pos = lax.broadcasted_iota(I32, (16, LANE), 0).astype(F32).astype(BF16)
    zero = jnp.zeros((16, LANE), BF16)
    one = jnp.ones((16, LANE), BF16)
    for q in range(PER):
        s = slice(LANE * q, LANE * (q + 1))
        val = val_of(first + q)
        hi = val.astype(BF16)
        lo = (val - hi.astype(F32)).astype(BF16)
        both = jnp.concatenate([hi, lo], 0)
        cell = cell_of(first + q)
        top = jnp.broadcast_to((cell >> 8).astype(F32), (16, LANE)).astype(BF16)
        rel = jnp.broadcast_to((cell & 255).astype(F32), (16, LANE)).astype(BF16) - pos
        for i in range(TOPS):
            A[16 * i:16 * i + 16, s] = jnp.where(top == BF16(i), both, zero)
        for i in range(BOTS // 16):
            B[16 * i:16 * i + 16, s] = jnp.where(rel == BF16(16 * i), one, zero)


def add_rows(first, rows, val_of, cell_of, A, B, ACC):
    def dot(p):
        ACC[...] += lax.dot_general(A[p][...], B[p][...], NT, preferred_element_type=F32)

    def step(s, _):
        base = first + 2 * PER * s
        build(base + PER, val_of, cell_of, A[1], B[1])
        dot(0)
        build(base + 2 * PER, val_of, cell_of, A[0], B[0])
        dot(1)
        return 0

    lax.fori_loop(0, rows // (2 * PER), step, 0)


def remote(src, dst, send, recv, i, d):
    return pltpu.make_async_remote_copy(
        src_ref=src,
        dst_ref=dst,
        send_sem=send.at[i],
        recv_sem=recv.at[i],
        device_id={"bl": d},
        device_id_type=MESH,
    )


def local_kernel(side, seq, pairs, w, vis, jones, cells_t, VAL, CR, CU, WC, WQ, V, G, Q, CB, WR):
    for j in range(cells_t.shape[1] // LANE):
        blk = cells_t[:, LANE * j:LANE * (j + 1)]
        CB[LANE * j:LANE * (j + 1), :] = jnp.transpose(jnp.concatenate([blk, blk], 0))
    stage(side, seq, pairs, w, vis, jones, V, G, Q, CB, CR, CU, WR, WC)
    stage_stokes(V, G, Q, WR, WQ, VAL)


def spread(row):
    return jnp.broadcast_to(row.astype(F32), (16, LANE)).astype(BF16)


def weigh_cells(CT, W4, HS, HB):
    pos = lax.broadcasted_iota(I32, (16, LANE), 0).astype(F32).astype(BF16)
    zero = jnp.zeros((16, LANE), BF16)
    one = jnp.ones((16, LANE), BF16)
    high = HB.shape[0]
    pitch = high + 8

    def body(g, _):
        weight = spread(W4[pl.ds(g // 4, 1), :])
        for q in range(16):
            cell = CT[pl.ds(16 * g + q, 1), :]
            up = spread(cell >> 7) - pos
            along = spread(cell & 127) - pos
            left = jnp.concatenate([jnp.where(up == BF16(16 * i), weight, zero) for i in range(high // 16)], 0)
            right = jnp.concatenate([jnp.where(along == BF16(16 * i), one, zero) for i in range(8)], 0)
            HS[pitch * q:pitch * q + high, :] = lax.dot_general(left, right, NT, preferred_element_type=F32)
        for u in range(high):
            x = jnp.concatenate([HS[pl.ds(u, 8, stride=pitch), :], HS[pl.ds(u + 8 * pitch, 8, stride=pitch), :]], 0)
            hi = x.astype(BF16)
            HB[u, pl.ds(16 * g, 16), 0:LANE] = hi
            HB[u, pl.ds(16 * g, 16), LANE:2 * LANE] = (x - hi.astype(F32)).astype(BF16)
        return 0

    lax.fori_loop(0, CT.shape[0] // 16, body, 0)


def whole_kernel(n, side, scale, VAL, CR, CU, WC, WQ, sky, means, PC, PW, X, XW, Y, YW, R1, RA, T, U,
                 ACC, A0, B0, A1, B1, CT, WT, W4, HS, HB, GR, PG, HA, K, L, send, recv):
    me = lax.axis_index("bl")
    core = lax.rem(me, 2)
    chip = me // 2
    x = chip // side
    y = lax.rem(chip, side)
    mate = 2 * chip + 1 - core
    first = x + core * (y - x)
    second = y + core * (x - y)
    step1 = 2 * side + core * (2 - 2 * side)
    step2 = 2 + core * (2 * side - 2)
    rows = CR.shape[0]

    def on_first(k):
        place = lax.rem(first + k, side)
        return place, me + (place - first) * step1

    def on_second(k):
        place = lax.rem(second + k, side)
        return place, me + (place - second) * step2

    def landed(ref, i):
        remote(ref, ref, send, recv, i, mate).wait_recv()

    def sent(ref, i):
        remote(ref, ref, send, recv, i, mate).wait_send()

    barrier = pltpu.get_barrier_semaphore()
    for k in range(1, side):
        for d in (on_first(k)[1], on_second(k)[1]):
            pl.semaphore_signal(barrier, inc=1, device_id={"bl": d}, device_id_type=MESH)
    pl.semaphore_signal(barrier, inc=1, device_id={"bl": mate}, device_id_type=MESH)
    pl.semaphore_wait(barrier, 2 * side - 1)

    remote(CU.at[1 - core], PC, send, recv, 0, mate).start()
    remote(WC.at[1 - core], PW, send, recv, 3, mate).start()
    remote(VAL.at[1 - core], R1, send, recv, 6, mate).start()

    def own_val(r):
        r = lax.rem(r, rows)
        unit = r // 2
        half = rows // 4
        at = pl.multiple_of(8 * lax.rem(r, 2), 8)
        return VAL[unit // half, lax.rem(unit, half) // side, lax.rem(unit, side), pl.ds(at, 8), :] * WQ[pl.ds(r, 1), :]

    def own_cell(r):
        return CR[pl.ds(lax.rem(r, rows), 1), :]

    bufs = (A0, A1), (B0, B1)
    ACC[...] = jnp.zeros_like(ACC)
    build(0, own_val, own_cell, A0, B0)
    landed(PC, 0)
    landed(PW, 3)
    for k in range(1, side):
        place, d = on_first(k)
        remote(CU.at[core, place], X.at[0, k], send, recv, 1, d).start()
        remote(PC.at[place], X.at[1, k], send, recv, 1, d).start()
        remote(WC.at[core], XW.at[0, k], send, recv, 4, d).start()
        remote(PW, XW.at[1, k], send, recv, 4, d).start()
    X[0, 0] = CU[core, first]
    X[1, 0] = PC[first]
    XW[0, 0] = WC[core]
    XW[1, 0] = PW[...]
    landed(R1, 6)

    def fold(i, _):
        R1[i] = R1[i] + VAL[core, i]
        return 0

    lax.fori_loop(0, side, fold, 0)
    for k in range(1, side):
        place, d = on_first(k)
        remote(R1.at[place], RA.at[k - 1], send, recv, 7, d).start()
    add_rows(0 * rows // 8, 4 * rows // 8, own_val, own_cell, *bufs, ACC)
    landed(X.at[:, 1:side], 1)
    landed(XW.at[:, 1:side], 4)
    for k in range(1, side):
        place, d = on_second(k)
        remote(X.at[:, :, place], Y.at[k], send, recv, 2, d).start()
        remote(XW, YW.at[k], send, recv, 5, d).start()
    Y[0] = X[:, :, second]
    YW[0] = XW[...]
    add_rows(4 * rows // 8, 1 * rows // 8, own_val, own_cell, *bufs, ACC)
    landed(RA, 7)
    for i in range(side):
        t = R1[first, i]
        for k in range(side - 1):
            t = t + RA[k, i]
        T[i] = t
    for k in range(1, side):
        place, d = on_second(k)
        remote(T.at[place], U.at[k - 1], send, recv, 8, d).start()
    add_rows(5 * rows // 8, 3 * rows // 8, own_val, own_cell, *bufs, ACC)
    landed(Y.at[1:side], 2)
    landed(YW.at[1:side], 5)
    for j in range(2):
        CT[LANE * j:LANE * (j + 1), :] = jnp.transpose(Y[:, :, :, j, :].reshape(n, LANE))
    for h in range(2):
        WT[...] = jnp.transpose(YW[:, :, :, h, :].reshape(n, LANE))
        for j in range(2):
            W4[2 * j + h:2 * j + h + 1, :] = WT[pl.ds(2 * side * first + 2 * second + j, 1), :]
    weigh_cells(CT, W4, HS, HB)
    landed(U, 8)

    total = T[second] + jnp.sum(U[...], axis=0)
    low = lax.broadcasted_iota(I32, (1, LANE), 1) < 64
    weights = jnp.sum(W4[...], axis=1, keepdims=True)
    averages = []
    for j in range(2):
        m = total[8 * j:8 * j + 8] / jnp.where(low, weights[2 * j:2 * j + 1], weights[2 * j + 1:2 * j + 2])
        averages.append(m)
        z = interleave(m)
        means[2 * j] = z[0:4]
        means[2 * j + 1] = z[4:8]
    m = jnp.concatenate(averages, 1)
    hi = m.astype(BF16)
    lo = (m - hi.astype(F32)).astype(BF16)
    left = jnp.concatenate([hi, lo], 0)
    for u in range(HB.shape[0]):
        both = jnp.dot(left, HB[u], preferred_element_type=F32)
        both = both[0:8] + both[8:16]
        i, h = u // 2, u % 2
        s = slice(LANE * h, LANE * (h + 1))
        z = ACC[16 * i:16 * i + 8, s] + ACC[16 * i + 8:16 * i + 16, s] - (both[:, :LANE] + both[:, LANE:])
        z = interleave(z) * scale
        for e in range(2):
            d = 2 * u + e
            at = (d // 2 // side, d // 2 % side) if e == 0 else (d // 2 % side, d // 2 // side)
            GR[e, at[0], at[1]] = z[4 * e:4 * e + 4]

    remote(GR.at[1 - core], PG, send, recv, 9, mate).start()
    landed(PG, 9)
    PG[...] = PG[...] + GR[core]
    for k in range(1, side):
        place, d = on_first(k)
        remote(PG.at[place], HA.at[k - 1], send, recv, 10, d).start()
    landed(HA, 10)
    K[...] = PG[first] + jnp.sum(HA[...], axis=0)
    for k in range(1, side):
        place, d = on_second(k)
        remote(K.at[place], L.at[k - 1], send, recv, 11, d).start()
    landed(L, 11)
    sky[0] = K[second] + jnp.sum(L[...], axis=0)
    for ref, i in (
        (PC, 0), (X.at[:, 1:side], 1), (Y.at[1:side], 2), (PW, 3), (XW.at[:, 1:side], 4), (YW.at[1:side], 5),
        (R1, 6), (RA, 7), (U, 8), (PG, 9), (HA, 10), (L, 11),
    ):
        sent(ref, i)


def per_device(n, vis, weight, cells, jones, pairs, seq):
    side = math.isqrt(n // 2)
    nb = weight.shape[1]
    rows = nb // 2
    sds = jax.ShapeDtypeStruct
    scale = math.sqrt(n * V_CELLS / (n * nb * cells.shape[2]))

    def vm(*shape, dtype=F32):
        return pltpu.VMEM(shape, dtype)

    tall = TOPS * 16
    val, *staged = pl.pallas_call(
        functools.partial(local_kernel, side),
        out_shape=(
            sds((4 * nb, LANE), F32),
            sds((rows, LANE), I32),
            sds((2, side, side, 2, LANE), I32),
            sds((2, 2, LANE), F32),
            sds((rows, LANE), F32),
        ),
        in_specs=[SMEM] * 3 + [VMEM] * 3,
        out_specs=(VMEM,) * 5,
        scratch_shapes=[vm(4 * nb, LANE)] * 3 + [vm(nb, LANE, dtype=I32), vm(rows, LANE)],
        compiler_params=pltpu.CompilerParams(vmem_limit_bytes=12 * MIB),
    )(seq, pairs, weight, vis.reshape(4 * nb, LANE), jones.reshape(-1, LANE), jnp.swapaxes(cells[0], 0, 1))
    sky, means = pl.pallas_call(
        functools.partial(whole_kernel, n, side, scale),
        out_shape=(sds((1, 4, LANE), F32), sds((4, 4, LANE), F32)),
        in_specs=[VMEM] * 5,
        out_specs=(VMEM, VMEM),
        scratch_shapes=[vm(side, side, 2, LANE, dtype=I32), vm(2, LANE)]
        + [vm(2, side, side, 2, LANE, dtype=I32), vm(2, side, 2, LANE)]
        + [vm(side, 2, side, 2, LANE, dtype=I32), vm(side, 2, side, 2, LANE)]
        + [vm(side, side, 16, LANE), vm(side - 1, side, 16, LANE), vm(side, 16, LANE), vm(side - 1, 16, LANE)]
        + [vm(tall, BOTS)]
        + [vm(tall, LANE * PER, dtype=BF16), vm(BOTS, LANE * PER, dtype=BF16)] * 2
        + [vm(rows, LANE, dtype=I32), vm(n, LANE), vm(4, LANE)]
        + [vm(16 * (n // 2 + 8), LANE), vm(n // 2, rows, 2 * LANE, dtype=BF16)]
        + [vm(2, side, side, 4, LANE), vm(side, side, 4, LANE), vm(side - 1, side, 4, LANE)]
        + [vm(side, 4, LANE), vm(side - 1, 4, LANE)]
        + [pltpu.SemaphoreType.DMA((12,))] * 2,
        compiler_params=pltpu.CompilerParams(collective_id=0, has_side_effects=True, vmem_limit_bytes=32 * MIB),
    )(val.reshape(2, side, side, 16, LANE), *staged)
    return sky, means


def solution(mesh):
    both = ("grp", "bl")
    return jax.shard_map(
        functools.partial(per_device, mesh.shape["bl"]),
        mesh=mesh,
        in_specs=(P(both, None, None, None), P(both, None), P(both, None, None), P(), P("grp", None), P("grp")),
        out_specs=(P(both, None, None), P(both, None, None)),
        check_vma=False,
    )
```
